768 devices in a mesh: ctx: 48 (over y, z_lo), head: 16 (over z_hi, x, core).
Axes of the slice: x: 4, y: 8, z: 12 (z_hi: 2, z_lo: 6; z = z_hi * 6 + z_lo), core: 2. Of those that a mesh axis runs over, the one named last changes fastest.
Arguments:
- queries: bfloat16 [12288, 8192], P('ctx', 'head'), may hold values from -15 to 15
- keys: bfloat16 [12288, 1024], P('ctx'), may hold values from -6 to 6
- values: bfloat16 [12288, 1024], P('ctx'), may hold values from -6 to 6
Outputs:
- attended: bfloat16 [12288, 8192], P('ctx', 'head')
The draws below stay inside these ranges and needn't reach their ends.
All inputs are finite; a program needn't handle non-finite values.
Results may differ from the reference program's by a relative error of at most 0.015.
Values may be sent and summed in bfloat16 or wider, within the bound.
A program may use at most 128 MiB of HBM per device.

```python
import math
import jax
import jax.numpy as jnp
from jax import lax

H = 64
KVH = 8
HD = 128
TOKENS = 12288


def draw_queries(key, part):
    noise_key = jax.random.fold_in(key, 1)
    base_rows = jax.random.normal(noise_key, (TOKENS, H * HD), jnp.float32)
    drawn = jnp.clip(2.5 * base_rows, -15.0, 15.0)
    return drawn.astype(jnp.bfloat16)


def draw_keys(key, part):
    noise_key = jax.random.fold_in(key, 2)
    base_rows = jax.random.normal(noise_key, (TOKENS, KVH * HD), jnp.float32)
    drawn = jnp.clip(base_rows, -6.0, 6.0)
    return drawn.astype(jnp.bfloat16)


def level_of(own_key, dims, cuts, smallest, high):
    gain, own = 1.0, jax.random.fold_in(own_key, 6)
    for dim, shards_of in cuts:
        heights = jnp.exp(jax.random.uniform(jax.random.fold_in(own, dim), (shards_of,), jnp.float32, smallest / len(cuts), high / len(cuts)))
        gain = gain * jnp.repeat(heights, dims[dim] // shards_of).reshape([-1 if axis == dim else 1 for axis in range(len(dims))])
    return gain


def gaussian(stream_key, extent, scale, limit, cuts=(), kind=jnp.bfloat16):
    gain = level_of(stream_key, extent, cuts, -0.22, 0.18) if cuts else 1.0
    entries = jax.random.normal(stream_key, extent, jnp.float32) * scale * gain
    return jnp.minimum(jnp.maximum(entries, -limit), limit).astype(kind)


def setup_inputs(seed: int = 0) -> dict:
    streams_of = jax.random.split(jax.random.key(seed), 4)
    queries = draw_queries(jax.random.fold_in(streams_of[3], 71), 0)
    keys = draw_keys(jax.random.fold_in(streams_of[3], 71), 0)
    values = gaussian(streams_of[2], (TOKENS, KVH * HD), 1.0, 6.0, ((0, 48),))
    return dict(queries=queries, keys=keys, values=values)


def reference(queries, keys, values):
    group_size = H // KVH
    block_rows = math.gcd(TOKENS, 512)
    block_count = TOKENS // block_rows
    grouped = queries.reshape(TOKENS, KVH, group_size, HD)
    keyed = keys.reshape(TOKENS, KVH, HD).astype(jnp.float32)
    valued = values.reshape(TOKENS, KVH, HD).astype(jnp.float32)
    key_pos = jnp.arange(TOKENS, dtype=jnp.int32)

    def one_block(block_index):
        block_start = (block_index // KVH) * block_rows
        kv_head = block_index % KVH
        zero_index = jnp.zeros((), jnp.int32)
        query_block = lax.dynamic_slice(grouped, (block_start, kv_head, zero_index, zero_index), (block_rows, 1, group_size, HD))[:, 0].astype(jnp.float32)
        key_head = lax.dynamic_slice_in_dim(keyed, kv_head, 1, 1)[:, 0]
        value_head = lax.dynamic_slice_in_dim(valued, kv_head, 1, 1)[:, 0]
        scores = jnp.einsum("qrd,kd->rqk", query_block, key_head, precision=lax.Precision.HIGHEST) * (HD ** -0.5)
        allowed = (block_start + jnp.arange(block_rows, dtype=jnp.int32))[:, None] >= key_pos[None, :]
        scores = jnp.where(allowed, scores, jnp.float32(-1e30))
        row_max = jnp.max(scores, axis=-1)
        weights = jnp.where(allowed, jnp.exp(scores - row_max[..., None]), jnp.float32(0.0))
        totals = jnp.sum(weights, axis=-1)
        rounded = lax.optimization_barrier(weights.astype(jnp.bfloat16)).astype(jnp.float32)
        result = jnp.einsum("rqk,kd->rqd", rounded, value_head, precision=lax.Precision.HIGHEST) / totals[..., None]
        return result.astype(jnp.bfloat16)

    stacked = lax.map(one_block, jnp.arange(block_count * KVH, dtype=jnp.int32))
    stacked = stacked.reshape(block_count, KVH, group_size, block_rows, HD)
    return jnp.transpose(stacked, (0, 3, 1, 2, 4)).reshape(TOKENS, H * HD)
```

```python
import functools
import jax
import jax.numpy as jnp
from jax import lax
from jax.experimental import pallas as pl
from jax.experimental.pallas import tpu as pltpu
from jax.sharding import PartitionSpec as P

H = 64
KVH = 8
HD = 128

NY = 8
NZ = 6
NX = 4
NH = 2

NEG = -1e30
LOG2E = 1.4426950408889634
MESH = pl.DeviceIdType.MESH


def kernel(q_hbm, k_hbm, v_hbm, o_ref, kv, stage, q_buf, qt, m_ref, l_ref, acc_ref,
           ld_sem, z_send, ring_send, sib_send, ici_recv, sib_recv, *, dims):
    ny, nz, nx = dims
    tok = q_hbm.shape[0]
    heads = q_hbm.shape[1] // HD
    half_z = nz // 2
    full = ny // 2
    span = half_z * tok

    ctx = lax.axis_index("ctx")
    head = lax.axis_index("head")
    y = ctx // nz
    zlo = ctx % nz
    core = head % 2
    x = (head // 2) % nx
    zhi = head // (2 * nx)
    z = zhi * nz + zlo
    ring_z = NH * nz

    def at_y(step):
        return {"ctx": lax.rem(y + step + ny, ny) * nz + zlo, "head": head}

    def at_z(step):
        there = lax.rem(z + step + ring_z, ring_z)
        hi = there // nz
        return {"ctx": y * nz + there % nz, "head": (hi * nx + x) * 2 + core}, hi

    sibling = {"ctx": ctx, "head": head + 1 - 2 * core}

    def columns(ref, g):
        return ref.at[:, pl.ds(pl.multiple_of(g * HD, HD), HD)]

    def chunk(kind, row, col):
        return kv.at[kind, row, pl.ds(pl.multiple_of(col * tok, tok), tok), :]

    g_own = zhi * nx + x

    @pl.when(core == 0)
    def _():
        for hi in range(NH):
            pltpu.make_async_copy(columns(k_hbm, hi * nx + x), stage.at[hi], ld_sem.at[hi]).start()

    @pl.when(core == 1)
    def _():
        for hi in range(NH):
            pltpu.make_async_copy(columns(v_hbm, hi * nx + x), stage.at[hi], ld_sem.at[hi]).start()

    own_k = pltpu.make_async_copy(columns(k_hbm, g_own), chunk(0, y, zlo), ld_sem.at[2])
    own_v = pltpu.make_async_copy(columns(v_hbm, g_own), chunk(1, y, zlo), ld_sem.at[3])
    own_q = pltpu.make_async_copy(q_hbm, q_buf, ld_sem.at[4])
    own_k.start()
    own_v.start()
    own_q.start()

    barrier = pltpu.get_barrier_semaphore()
    peers = [at_y(1), at_y(-1), sibling]
    for d in range(1, half_z + 1):
        peers.append(at_z(d)[0])
        peers.append(at_z(-d)[0])
    for peer in peers:
        pl.semaphore_signal(barrier, inc=1, device_id=peer, device_id_type=MESH)
    for hi in range(NH):
        pltpu.make_async_copy(stage.at[hi], stage.at[hi], ld_sem.at[hi]).wait()
    own_k.wait()
    own_v.wait()
    pl.semaphore_wait(barrier, len(peers))

    def ring_copy(row, col, way, step):
        return pltpu.make_async_remote_copy(
            src_ref=chunk(core, row, col), dst_ref=chunk(core, row, col),
            send_sem=ring_send.at[way, step, col], recv_sem=ici_recv.at[row, col],
            device_id=at_y(1 - 2 * way), device_id_type=MESH)

    def sib_copy(kind, row, col):
        return pltpu.make_async_remote_copy(
            src_ref=chunk(kind, row, col), dst_ref=chunk(kind, row, col),
            send_sem=sib_send.at[row, col], recv_sem=sib_recv.at[row, col],
            device_id=sibling, device_id_type=MESH)

    ring_copy(y, zlo, 0, 0).start()
    ring_copy(y, zlo, 1, 0).start()
    middle = half_z * (1 - 2 * core)
    steps_z = []
    for d in range(1, half_z):
        steps_z += [d, -d]
    steps_z.append(middle)
    z_copies = []
    for n, d in enumerate(steps_z):
        there, hi = at_z(d)
        z_copies.append(pltpu.make_async_remote_copy(
            src_ref=stage.at[hi], dst_ref=chunk(core, y, zlo),
            send_sem=z_send.at[n], recv_sem=ici_recv.at[y, zlo],
            device_id=there, device_id_type=MESH))
        z_copies[-1].start()

    own_q.wait()
    for h in range(heads):
        qt[h] = q_buf[:, h * HD:(h + 1) * HD].astype(jnp.float32).T.astype(jnp.bfloat16)
    m_ref[...] = jnp.full_like(m_ref, NEG)
    l_ref[...] = jnp.zeros_like(l_ref)
    acc_ref[...] = jnp.zeros_like(acc_ref)

    for d in steps_z:
        col = lax.rem(zlo - d + ring_z, nz)
        ring_copy(y, col, 0, 0).wait_recv()
        ring_copy(y, col, 0, 0).start()
        ring_copy(y, col, 1, 0).start()
        sib_copy(core, y, col).start()

    def where_is(item):
        i = jnp.maximum(item - 2, 0)
        step = jnp.where(item < 2, 0, 1 + i // 4)
        way = i % 2
        hf = jnp.where(item < 2, item, jnp.where(step == full, way, (i // 2) % 2))
        row = lax.rem(y + step * (2 * way - 1) + ny, ny)
        return step, way, hf, row

    def move(item):
        step, way, hf, row = where_is(item)
        onward = (step < full - 1) | ((step == full - 1) & (hf == way))
        for jj in range(half_z):
            col = hf * half_z + jj
            ring_copy(row, col, way, step).wait_recv()

            @pl.when(onward)
            def _():
                ring_copy(row, col, way, step).start()
            sib_copy(core, row, col).start()

    def attend(row, hf, masked):
        keys = kv[0, row, pl.ds(pl.multiple_of(hf * span, span), span), :]
        vals_t = kv[1, row, pl.ds(pl.multiple_of(hf * span, span), span), :].T
        scale = LOG2E * HD ** -0.5
        if masked:
            ahead = (lax.broadcasted_iota(jnp.int32, (span, tok), 0)
                     - lax.broadcasted_iota(jnp.int32, (span, tok), 1))
            allowed = ahead <= ctx * tok - (row * nz + hf * half_z) * tok

        def scores(h):
            s = jnp.dot(keys, qt[h], preferred_element_type=jnp.float32)
            return jnp.where(allowed, s, NEG) if masked else s

        s = scores(0)
        for h in range(heads):
            s_next = scores(h + 1) if h + 1 < heads else None
            old = m_ref[h]
            new = jnp.maximum(old, jnp.max(s, axis=0, keepdims=True))
            shrink = jnp.exp2((old - new) * scale)
            w = jnp.exp2((s - new) * scale)
            m_ref[h] = new
            l_ref[h] = l_ref[h] * shrink + jnp.sum(w, axis=0, keepdims=True)
            acc_ref[h] = acc_ref[h] * shrink + jnp.dot(
                vals_t, w.astype(jnp.bfloat16), preferred_element_type=jnp.float32)
            s = s_next

    n_items = 2 + 4 * (full - 1) + 2

    @pl.loop(1, n_items + 1)
    def _(it):
        @pl.when((it >= 2) & (it < n_items))
        def _():
            move(it)
        item = it - 1
        step, way, hf, row = where_is(item)
        for jj in range(half_z):
            col = hf * half_z + jj

            @pl.when((item >= 2) | (col != zlo))
            def _():
                sib_copy(1 - core, row, col).wait_recv()

        @pl.when((item < 2) & (hf * half_z <= zlo))
        def _():
            attend(row, hf, True)

        @pl.when((item >= 2) & (row < y))
        def _():
            attend(row, hf, False)

    for h in range(heads):
        out = (acc_ref[h] / l_ref[h]).T
        o_ref[:, h * HD:(h + 1) * HD] = out.astype(jnp.bfloat16)

    for copy in z_copies:
        copy.wait_send()

    @pl.loop(0, nz)
    def _(col):
        for way in range(2):
            for step in range(full - 1):
                ring_copy(y, col, way, step).wait_send()
            @pl.when((col // half_z) == way)
            def _():
                ring_copy(y, col, way, full - 1).wait_send()

    @pl.loop(0, ny)
    def _(row):
        @pl.loop(0, nz)
        def _(col):
            @pl.when((row != y) | (col != zlo))
            def _():
                sib_copy(core, row, col).wait_send()


def attention(queries, keys, values, dims):
    ny, nz, nx = dims
    tok = queries.shape[0]
    heads = queries.shape[1] // HD
    any_space = pl.BlockSpec(memory_space=pl.ANY)
    dma = pltpu.SemaphoreType.DMA
    return pl.pallas_call(
        functools.partial(kernel, dims=dims),
        out_shape=jax.ShapeDtypeStruct(queries.shape, jnp.bfloat16),
        in_specs=[any_space] * 3,
        out_specs=pl.BlockSpec(memory_space=pltpu.VMEM),
        scratch_shapes=[
            pltpu.VMEM((2, ny, nz * tok, HD), jnp.bfloat16),
            pltpu.VMEM((NH, tok, HD), jnp.bfloat16),
            pltpu.VMEM((tok, heads * HD), jnp.bfloat16),
            pltpu.VMEM((heads, HD, tok), jnp.bfloat16),
            pltpu.VMEM((heads, 1, tok), jnp.float32),
            pltpu.VMEM((heads, 1, tok), jnp.float32),
            pltpu.VMEM((heads, HD, tok), jnp.float32),
            dma((5,)),
            dma((nz - 1,)),
            dma((2, ny // 2, nz)),
            dma((ny, nz)),
            dma((ny, nz)),
            dma((ny, nz)),
        ],
        compiler_params=pltpu.CompilerParams(
            collective_id=0, has_side_effects=True, vmem_limit_bytes=48 * 1024 * 1024),
        name="causal_ring",
    )(queries, keys, values)


def solution(mesh):
    return jax.shard_map(
        functools.partial(attention, dims=(NY, NZ, NX)),
        mesh=mesh,
        in_specs=(P("ctx", "head"), P("ctx", None), P("ctx", None)),
        out_specs=P("ctx", "head"),
        check_vma=False,
    )
```

```python
import functools
import jax
import jax.numpy as jnp
from jax import lax
from jax.experimental import pallas as pl
from jax.experimental.pallas import tpu as pltpu
from jax.sharding import PartitionSpec as P

H = 64
KVH = 8
HD = 128

NY = 8
NZ = 6
NX = 4

SLOPE = 0.05
LAG = 1
AHEAD = 1

NEG = -1e30
LOG2E = 1.4426950408889634
MESH = pl.DeviceIdType.MESH


MATE, OWN = 0, 1


def plan(ny, places):
    full = ny // 2
    arrivals = sorted(((s, p) for s in range(full + 1) for p in range(places)),
                      key=lambda e: (SLOPE * e[1] + e[0], e[0]))
    blocks = [(s, way) for s in range(full + 1) for way in range(2 if 0 < s < full else 1)]
    ahead = min(AHEAD, len(blocks))
    order = ([(b, OWN) for b in blocks[:ahead]] + [(b, MATE) for b in blocks]
             + [(b, OWN) for b in blocks[ahead:]])
    needs, seen = [], set()
    for (s, way), _ in order:
        ready = max(n for n, e in enumerate(arrivals) if e[0] == s) + 1 + LAG
        needs.append(min(max([ready] + needs[-1:]), len(arrivals)))
    last = needs.index(len(arrivals))
    for n in range(1, last):
        even = needs[0] + (len(arrivals) - needs[0]) * n // last
        needs[n] = max(needs[n], min(even, needs[n] + 2))
    items = []
    for (block, whose), need in zip(order, needs):
        items.append((*block, whose, need, block not in seen))
        seen.add(block)
    return arrivals, items


def pick(index, values):
    out = jnp.int32(values[0])
    for n in range(1, len(values)):
        if values[n] != values[n - 1]:
            out = jnp.where(index >= n, values[n], out)
    return out


def kernel(q_hbm, k_hbm, v_hbm, o_ref, kv, q_buf, qt, m_ref, l_ref, acc_ref, part, stat,
           ld_sem, z_send, ring_send, sib_send, pair_send, ici_recv, sib_recv, pair_recv, *, dims):
    ny, nz, nx = dims
    tok = q_hbm.shape[0]
    heads = q_hbm.shape[1] // HD
    places = nz // 2
    full = ny // 2
    span = places * tok
    scale = LOG2E * HD ** -0.5
    arrivals, items = plan(ny, places)

    ctx = lax.axis_index("ctx")
    head = lax.axis_index("head")
    y = ctx // nz
    zlo = ctx % nz
    core = head % 2
    g_own = head // 2
    mate_z = zlo + 1 - 2 * (zlo % 2)

    def device(at_y, at_z):
        return {"ctx": at_y * nz + at_z, "head": head}

    below_y = device(lax.rem(y + ny - 1, ny), zlo)
    above_y = device(lax.rem(y + 1, ny), zlo)
    mate = device(y, mate_z)
    sibling = {"ctx": ctx, "head": head + 1 - 2 * core}

    def column(place):
        return lax.rem(zlo + 2 * place, nz)

    def chunk(kind, row, place):
        return kv.at[kind, row, pl.ds(pl.multiple_of(place * tok, tok), tok), :]

    def columns(ref):
        return ref.at[:, pl.ds(pl.multiple_of(g_own * HD, HD), HD)]

    own_k = pltpu.make_async_copy(columns(k_hbm), chunk(0, y, 0), ld_sem.at[0])
    own_v = pltpu.make_async_copy(columns(v_hbm), chunk(1, y, 0), ld_sem.at[1])
    own_q = pltpu.make_async_copy(q_hbm, q_buf.at[1], ld_sem.at[2])
    own_k.start()
    own_v.start()
    own_q.start()

    barrier = pltpu.get_barrier_semaphore()
    peers = [below_y, above_y, sibling, mate] + [device(y, column(p)) for p in range(1, places)]
    for peer in peers:
        pl.semaphore_signal(barrier, inc=1, device_id=peer, device_id_type=MESH)
    own_k.wait()
    own_v.wait()
    pl.semaphore_wait(barrier, len(peers))

    def along_y(row, place, way, step):
        return pltpu.make_async_remote_copy(
            src_ref=chunk(core, row, place), dst_ref=chunk(core, row, place),
            send_sem=ring_send.at[way, step, place], recv_sem=ici_recv.at[row, place],
            device_id=(above_y, below_y)[way], device_id_type=MESH)

    def along_z(place):
        return pltpu.make_async_remote_copy(
            src_ref=chunk(core, y, 0), dst_ref=chunk(core, y, places - place),
            send_sem=z_send.at[place], recv_sem=ici_recv.at[y, places - place],
            device_id=device(y, column(place)), device_id_type=MESH)

    def across(kind, row, place):
        return pltpu.make_async_remote_copy(
            src_ref=chunk(kind, row, place), dst_ref=chunk(kind, row, place),
            send_sem=sib_send.at[row, place], recv_sem=sib_recv.at[row, place],
            device_id=sibling, device_id_type=MESH)

    def to_mate(src, dst, n):
        return pltpu.make_async_remote_copy(
            src_ref=src, dst_ref=dst, send_sem=pair_send.at[n], recv_sem=pair_recv.at[n],
            device_id=mate, device_id_type=MESH)

    def last_way(place):
        return 0 if place < (places + 1) // 2 else 1

    def take_in(step, place):
        if step == 0:
            if place:
                along_y(y, place, 0, 0).wait_recv()
            along_y(y, place, 0, 0).start()
            along_y(y, place, 1, 0).start()
            if place:
                across(core, y, place).start()
            else:
                for other in range(1, places):
                    along_z(other).start()
            return
        for way in range(2):
            if step == full and last_way(place) != way:
                continue
            row = lax.rem(y + (step if way else ny - step), ny)
            along_y(row, place, way, step - 1).wait_recv()
            if step < full - 1 or (step == full - 1 and last_way(place) == way):
                along_y(row, place, way, step).start()
            across(core, row, place).start()

    def attend(row, whose, own_row):
        base = whose * heads
        keys = kv[0, row]
        vals_t = kv[1, row].T
        if own_row:
            ahead = (lax.broadcasted_iota(jnp.int32, (tok, tok), 0)
                     - lax.broadcasted_iota(jnp.int32, (tok, tok), 1))
            here = jnp.where(whose == OWN, zlo, mate_z)
            limits = [jnp.where(column(p) == here, 0, jnp.where(column(p) < here, tok, -tok))
                      for p in range(places)]
            allowed = jnp.concatenate([ahead <= t for t in limits], axis=0)

        def scores(h):
            s = jnp.dot(keys, qt[base + h], preferred_element_type=jnp.float32)
            return jnp.where(allowed, s, NEG) if own_row else s

        s = scores(0)
        for h in range(heads):
            s_next = scores(h + 1) if h + 1 < heads else None
            old = m_ref[base + h]
            new = jnp.maximum(old, jnp.max(s, axis=0, keepdims=True))
            shrink = jnp.exp2((old - new) * scale)
            w = jnp.exp2((s - new) * scale)
            m_ref[base + h] = new
            l_ref[base + h] = l_ref[base + h] * shrink + jnp.sum(w, axis=0, keepdims=True)
            acc_ref[base + h] = acc_ref[base + h] * shrink + jnp.dot(
                vals_t, w.astype(jnp.bfloat16), preferred_element_type=jnp.float32)
            s = s_next

    take_in(*arrivals[0])
    queries_over = to_mate(q_hbm, q_buf.at[MATE], 0)
    queries_over.start()

    def transpose_queries(whose):
        for h in range(heads):
            qt[whose * heads + h] = q_buf[whose, :, h * HD:(h + 1) * HD].astype(
                jnp.float32).T.astype(jnp.bfloat16)

    own_q.wait()
    transpose_queries(OWN)
    m_ref[...] = jnp.full_like(m_ref, NEG)
    l_ref[...] = jnp.zeros_like(l_ref)
    acc_ref[...] = jnp.zeros_like(acc_ref)

    returns = [to_mate(part.at[0, h], part.at[1, h], 1 + h) for h in range(heads)]
    stats_over = to_mate(stat.at[0], stat.at[1], 1 + heads)
    whose_of = [item[2] for item in items]
    first_mate = whose_of.index(MATE)
    after_mate = first_mate + whose_of.count(MATE)

    def send_back():
        for h in range(heads):
            part[0, h] = acc_ref[h].astype(jnp.bfloat16)
            stat[0, h] = m_ref[h]
            stat[0, heads + h] = l_ref[h]
        stats_over.start()
        for copy in returns:
            copy.start()

    @pl.loop(0, len(items))
    def _(n):
        done = 1
        for i, item in enumerate(items):
            if item[3] > done:
                first, done = done, item[3]

                @pl.when(n == i)
                def _():
                    for arrival in arrivals[first:item[3]]:
                        take_in(*arrival)

        @pl.when(n == first_mate)
        def _():
            queries_over.wait_recv()
            transpose_queries(MATE)

        if after_mate < len(items):
            @pl.when(n == after_mate)
            def _():
                send_back()
        step = pick(n, [b[0] for b in items])
        way = pick(n, [b[1] for b in items])
        whose = pick(n, whose_of)
        fresh = pick(n, [int(b[4]) for b in items]) == 1
        row = lax.rem(y + jnp.where(way == 1, step, ny - step), ny)
        for place in range(places):
            @pl.when((row != y) & fresh if place == 0 else fresh)
            def _():
                across(1 - core, row, place).wait_recv()

        @pl.when(row == y)
        def _():
            attend(row, whose, True)

        @pl.when(row < y)
        def _():
            attend(row, whose, False)

    if after_mate == len(items):
        send_back()

    queries_over.wait_send()

    @pl.loop(0, places)
    def _(place):
        @pl.when(place > 0)
        def _():
            along_z(place).wait_send()
        for way in range(2):
            for step in range(full - 1):
                along_y(y, place, way, step).wait_send()

            @pl.when((place >= (places + 1) // 2) == (way == 1))
            def _():
                along_y(y, place, way, full - 1).wait_send()

    @pl.loop(0, ny)
    def _(row):
        for place in range(places):
            if place == 0:
                @pl.when(row != y)
                def _():
                    across(core, row, place).wait_send()
            else:
                across(core, row, place).wait_send()

    stats_over.wait_recv()
    for h in range(heads):
        returns[h].wait_recv()
        m_own, m_in = m_ref[heads + h], stat[1, h]
        top = jnp.maximum(m_own, m_in)
        a, b = jnp.exp2((m_own - top) * scale), jnp.exp2((m_in - top) * scale)
        total = l_ref[heads + h] * a + stat[1, heads + h] * b
        out = (acc_ref[heads + h] * a + part[1, h].astype(jnp.float32) * b) / total
        o_ref[:, h * HD:(h + 1) * HD] = out.T.astype(jnp.bfloat16)
    stats_over.wait_send()
    for copy in returns:
        copy.wait_send()


def attention(queries, keys, values, dims):
    ny, nz, nx = dims
    tok = queries.shape[0]
    heads = queries.shape[1] // HD
    places = nz // 2
    any_space = pl.BlockSpec(memory_space=pl.ANY)
    dma = pltpu.SemaphoreType.DMA
    return pl.pallas_call(
        functools.partial(kernel, dims=dims),
        out_shape=jax.ShapeDtypeStruct(queries.shape, jnp.bfloat16),
        in_specs=[any_space] * 3,
        out_specs=pl.BlockSpec(memory_space=pltpu.VMEM),
        scratch_shapes=[
            pltpu.VMEM((2, ny, places * tok, HD), jnp.bfloat16),
            pltpu.VMEM((2, tok, heads * HD), jnp.bfloat16),
            pltpu.VMEM((2 * heads, HD, tok), jnp.bfloat16),
            pltpu.VMEM((2 * heads, 1, tok), jnp.float32),
            pltpu.VMEM((2 * heads, 1, tok), jnp.float32),
            pltpu.VMEM((2 * heads, HD, tok), jnp.float32),
            pltpu.VMEM((2, heads, HD, tok), jnp.bfloat16),
            pltpu.VMEM((2, 2 * heads, 1, tok), jnp.float32),
            dma((3,)),
            dma((places,)),
            dma((2, ny // 2, places)),
            dma((ny, places)),
            dma((heads + 2,)),
            dma((ny, places)),
            dma((ny, places)),
            dma((heads + 2,)),
        ],
        compiler_params=pltpu.CompilerParams(
            collective_id=0, has_side_effects=True, vmem_limit_bytes=67043328),
        name="causal_ring",
    )(queries, keys, values)


def solution(mesh):
    return jax.shard_map(
        functools.partial(attention, dims=(NY, NZ, NX)),
        mesh=mesh,
        in_specs=(P("ctx", "head"), P("ctx", None), P("ctx", None)),
        out_specs=P("ctx", "head"),
        check_vma=False,
    )
```

```python
import functools
import jax
import jax.numpy as jnp
from jax import lax
from jax.experimental import pallas as pl
from jax.experimental.pallas import tpu as pltpu
from jax.sharding import PartitionSpec as P

H = 64
KVH = 8
HD = 128

NY = 8
NZ = 6
NX = 4

SLOPE = 0.05
LAG = 1
AHEAD = 1

NEG = -1e30
LOG2E = 1.4426950408889634
MESH = pl.DeviceIdType.MESH


MATE, OWN = 0, 1


def plan(ny, places):
    full = ny // 2
    arrivals = sorted(((s, p) for s in range(full + 1) for p in range(places)),
                      key=lambda e: (SLOPE * e[1] + e[0], e[0]))
    blocks = [(s, way) for s in range(full + 1) for way in range(2 if 0 < s < full else 1)]
    ahead = min(AHEAD, len(blocks))
    order = ([(b, OWN) for b in blocks[:ahead]] + [(b, MATE) for b in blocks]
             + [(b, OWN) for b in blocks[ahead:]])
    needs, seen = [], set()
    for (s, way), _ in order:
        ready = max(n for n, e in enumerate(arrivals) if e[0] == s) + 1 + LAG
        needs.append(min(max([ready] + needs[-1:]), len(arrivals)))
    last = needs.index(len(arrivals))
    for n in range(1, last):
        even = needs[0] + (len(arrivals) - needs[0]) * n // last
        needs[n] = max(needs[n], min(even, needs[n] + 2))
    items = []
    for (block, whose), need in zip(order, needs):
        items.append((*block, whose, need, block not in seen))
        seen.add(block)
    return arrivals, items


def pick(index, values):
    out = jnp.int32(values[0])
    for n in range(1, len(values)):
        if values[n] != values[n - 1]:
            out = jnp.where(index >= n, values[n], out)
    return out


def kernel(q_hbm, k_hbm, v_hbm, o_ref, kv, q_buf, qt, m_ref, l_ref, acc_ref, part, stat,
           ld_sem, z_send, ring_send, sib_send, pair_send, ici_recv, sib_recv, pair_recv, *, dims):
    ny, nz, nx = dims
    tok = q_hbm.shape[0]
    heads = q_hbm.shape[1] // HD
    places = nz // 2
    full = ny // 2
    span = places * tok
    scale = LOG2E * HD ** -0.5
    arrivals, items = plan(ny, places)

    ctx = lax.axis_index("ctx")
    head = lax.axis_index("head")
    y = ctx // nz
    zlo = ctx % nz
    core = head % 2
    g_own = head // 2
    mate_z = zlo + 1 - 2 * (zlo % 2)

    def device(at_y, at_z):
        return {"ctx": at_y * nz + at_z, "head": head}

    below_y = device(lax.rem(y + ny - 1, ny), zlo)
    above_y = device(lax.rem(y + 1, ny), zlo)
    mate = device(y, mate_z)
    sibling = {"ctx": ctx, "head": head + 1 - 2 * core}

    def column(place):
        return lax.rem(zlo + 2 * place, nz)

    def chunk(kind, row, place):
        return kv.at[kind, row, pl.ds(pl.multiple_of(place * tok, tok), tok), :]

    def columns(ref):
        return ref.at[:, pl.ds(pl.multiple_of(g_own * HD, HD), HD)]

    own_k = pltpu.make_async_copy(columns(k_hbm), chunk(0, y, 0), ld_sem.at[0])
    own_v = pltpu.make_async_copy(columns(v_hbm), chunk(1, y, 0), ld_sem.at[1])
    own_q = pltpu.make_async_copy(q_hbm, q_buf.at[1], ld_sem.at[2])
    own_k.start()
    own_v.start()
    own_q.start()

    barrier = pltpu.get_barrier_semaphore()
    peers = [below_y, above_y, sibling, mate] + [device(y, column(p)) for p in range(1, places)]
    for peer in peers:
        pl.semaphore_signal(barrier, inc=1, device_id=peer, device_id_type=MESH)
    own_k.wait()
    own_v.wait()
    pl.semaphore_wait(barrier, len(peers))

    def along_y(row, place, way, step):
        return pltpu.make_async_remote_copy(
            src_ref=chunk(core, row, place), dst_ref=chunk(core, row, place),
            send_sem=ring_send.at[way, step, place], recv_sem=ici_recv.at[row, place],
            device_id=(above_y, below_y)[way], device_id_type=MESH)

    def along_z(place):
        return pltpu.make_async_remote_copy(
            src_ref=chunk(core, y, 0), dst_ref=chunk(core, y, places - place),
            send_sem=z_send.at[place], recv_sem=ici_recv.at[y, places - place],
            device_id=device(y, column(place)), device_id_type=MESH)

    def across(kind, row, place):
        return pltpu.make_async_remote_copy(
            src_ref=chunk(kind, row, place), dst_ref=chunk(kind, row, place),
            send_sem=sib_send.at[row, place], recv_sem=sib_recv.at[row, place],
            device_id=sibling, device_id_type=MESH)

    def to_mate(src, dst, n):
        return pltpu.make_async_remote_copy(
            src_ref=src, dst_ref=dst, send_sem=pair_send.at[n], recv_sem=pair_recv.at[n],
            device_id=mate, device_id_type=MESH)

    def last_way(place):
        return jnp.where(2 * place + 1 == places, core, jnp.where(2 * place < places, 0, 1))

    def take_in(step, place):
        if step == 0:
            if place:
                along_y(y, place, 0, 0).wait_recv()
            along_y(y, place, 0, 0).start()
            along_y(y, place, 1, 0).start()
            if place:
                across(core, y, place).start()
            else:
                for other in range(1, places):
                    along_z(other).start()
            return
        for way in range(2):
            if step == full and way:
                continue
            row = lax.rem(y + (step if way else ny - step), ny)
            along_y(row, place, way, step - 1).wait_recv()
            if step < full - 1:
                along_y(row, place, way, step).start()
            elif step == full - 1:
                @pl.when(last_way(place) == way)
                def _():
                    along_y(row, place, way, step).start()
            across(core, row, place).start()

    def attend(row, whose, own_row):
        base = whose * heads
        keys = kv[0, row]
        vals_t = kv[1, row].T
        if own_row:
            ahead = (lax.broadcasted_iota(jnp.int32, (tok, tok), 0)
                     - lax.broadcasted_iota(jnp.int32, (tok, tok), 1))
            here = jnp.where(whose == OWN, zlo, mate_z)
            limits = [jnp.where(column(p) == here, 0, jnp.where(column(p) < here, tok, -tok))
                      for p in range(places)]
            allowed = jnp.concatenate([ahead <= t for t in limits], axis=0)

        def scores(h):
            s = jnp.dot(keys, qt[base + h], preferred_element_type=jnp.float32)
            return jnp.where(allowed, s, NEG) if own_row else s

        s = scores(0)
        for h in range(heads):
            s_next = scores(h + 1) if h + 1 < heads else None
            old = m_ref[base + h]
            new = jnp.maximum(old, jnp.max(s, axis=0, keepdims=True))
            shrink = jnp.exp2((old - new) * scale)
            w = jnp.exp2((s - new) * scale)
            m_ref[base + h] = new
            l_ref[base + h] = l_ref[base + h] * shrink + jnp.sum(w, axis=0, keepdims=True)
            acc_ref[base + h] = acc_ref[base + h] * shrink + jnp.dot(
                vals_t, w.astype(jnp.bfloat16), preferred_element_type=jnp.float32)
            s = s_next

    take_in(*arrivals[0])
    queries_over = to_mate(q_hbm, q_buf.at[MATE], 0)
    queries_over.start()

    def transpose_queries(whose):
        for h in range(heads):
            qt[whose * heads + h] = q_buf[whose, :, h * HD:(h + 1) * HD].astype(
                jnp.float32).T.astype(jnp.bfloat16)

    own_q.wait()
    transpose_queries(OWN)
    m_ref[...] = jnp.full_like(m_ref, NEG)
    l_ref[...] = jnp.zeros_like(l_ref)
    acc_ref[...] = jnp.zeros_like(acc_ref)

    returns = [to_mate(part.at[0, h], part.at[1, h], 1 + h) for h in range(heads)]
    stats_over = to_mate(stat.at[0], stat.at[1], 1 + heads)
    whose_of = [item[2] for item in items]
    first_mate = whose_of.index(MATE)
    after_mate = first_mate + whose_of.count(MATE)

    def send_back():
        for h in range(heads):
            stat[0, h] = m_ref[h]
            stat[0, heads + h] = l_ref[h]
        part[0, 0] = acc_ref[0].astype(jnp.bfloat16)
        stats_over.start()
        for h in range(1, heads):
            part[0, h] = acc_ref[h].astype(jnp.bfloat16)
            returns[h - 1].start()
        returns[heads - 1].start()

    @pl.loop(0, len(items))
    def _(n):
        done = 1
        for i, item in enumerate(items):
            if item[3] > done:
                first, done = done, item[3]

                @pl.when(n == i)
                def _():
                    for arrival in arrivals[first:item[3]]:
                        take_in(*arrival)

        @pl.when(n == first_mate)
        def _():
            queries_over.wait_recv()
            transpose_queries(MATE)

        if after_mate < len(items):
            @pl.when(n == after_mate)
            def _():
                send_back()
        step = pick(n, [b[0] for b in items])
        way = pick(n, [b[1] for b in items])
        whose = pick(n, whose_of)
        fresh = pick(n, [int(b[4]) for b in items]) == 1
        row = lax.rem(y + jnp.where(way == 1, step, ny - step), ny)
        for place in range(places):
            @pl.when((row != y) & fresh if place == 0 else fresh)
            def _():
                across(1 - core, row, place).wait_recv()

        @pl.when(row == y)
        def _():
            attend(row, whose, True)

        @pl.when(row < y)
        def _():
            attend(row, whose, False)

    if after_mate == len(items):
        send_back()

    queries_over.wait_send()

    @pl.loop(0, places)
    def _(place):
        @pl.when(place > 0)
        def _():
            along_z(place).wait_send()
        for way in range(2):
            for step in range(full - 1):
                along_y(y, place, way, step).wait_send()

            @pl.when(last_way(place) == way)
            def _():
                along_y(y, place, way, full - 1).wait_send()

    @pl.loop(0, ny)
    def _(row):
        for place in range(places):
            if place == 0:
                @pl.when(row != y)
                def _():
                    across(core, row, place).wait_send()
            else:
                across(core, row, place).wait_send()

    stats_over.wait_recv()
    for h in range(heads):
        returns[h].wait_recv()
        m_own, m_in = m_ref[heads + h], stat[1, h]
        top = jnp.maximum(m_own, m_in)
        a, b = jnp.exp2((m_own - top) * scale), jnp.exp2((m_in - top) * scale)
        total = l_ref[heads + h] * a + stat[1, heads + h] * b
        out = (acc_ref[heads + h] * a + part[1, h].astype(jnp.float32) * b) / total
        o_ref[:, h * HD:(h + 1) * HD] = out.T.astype(jnp.bfloat16)
    stats_over.wait_send()
    for copy in returns:
        copy.wait_send()


def attention(queries, keys, values, dims):
    ny, nz, nx = dims
    tok = queries.shape[0]
    heads = queries.shape[1] // HD
    places = nz // 2
    any_space = pl.BlockSpec(memory_space=pl.ANY)
    dma = pltpu.SemaphoreType.DMA
    return pl.pallas_call(
        functools.partial(kernel, dims=dims),
        out_shape=jax.ShapeDtypeStruct(queries.shape, jnp.bfloat16),
        in_specs=[any_space] * 3,
        out_specs=pl.BlockSpec(memory_space=pltpu.VMEM),
        scratch_shapes=[
            pltpu.VMEM((2, ny, places * tok, HD), jnp.bfloat16),
            pltpu.VMEM((2, tok, heads * HD), jnp.bfloat16),
            pltpu.VMEM((2 * heads, HD, tok), jnp.bfloat16),
            pltpu.VMEM((2 * heads, 1, tok), jnp.float32),
            pltpu.VMEM((2 * heads, 1, tok), jnp.float32),
            pltpu.VMEM((2 * heads, HD, tok), jnp.float32),
            pltpu.VMEM((2, heads, HD, tok), jnp.bfloat16),
            pltpu.VMEM((2, 2 * heads, 1, tok), jnp.float32),
            dma((3,)),
            dma((places,)),
            dma((2, ny // 2, places)),
            dma((ny, places)),
            dma((heads + 2,)),
            dma((ny, places)),
            dma((ny, places)),
            dma((heads + 2,)),
        ],
        compiler_params=pltpu.CompilerParams(
            collective_id=0, has_side_effects=True, vmem_limit_bytes=67043328),
        name="causal_ring",
    )(queries, keys, values)


def solution(mesh):
    return jax.shard_map(
        functools.partial(attention, dims=(NY, NZ, NX)),
        mesh=mesh,
        in_specs=(P("ctx", "head"), P("ctx", None), P("ctx", None)),
        out_specs=P("ctx", "head"),
        check_vma=False,
    )
```
